128 devices in a mesh: el: 8 (over y, x_lo), ph: 16 (over x_hi, z, core).
Axes of the slice: x: 4 (x_hi: 2, x_lo: 2; x = x_hi * 2 + x_lo), y: 4, z: 4, core: 2. Of those that a mesh axis runs over, the one named last changes fastest.
Arguments:
- elec_dev: float32 [128, 96, 256], P(('el', 'ph')), may hold values from -6 to 6
- phon_dev: float32 [16, 24, 96, 256], P('ph', 'el'), may hold values from -6 to 6
- elec_source: float32 [128, 96, 256], P(('el', 'ph')), may hold values from -6 to 6
- phon_source: float32 [16, 24, 96, 256], P('ph', 'el'), may hold values from -6 to 6
- elec_rate: float32 [128, 256], P(('el', 'ph')), may hold values from 0.75 to 3
- phon_rate: float32 [16, 24, 256], P('ph', 'el'), may hold values from 0.75 to 3
- tiles: bfloat16 [8, 16, 128, 256, 256], P('el', 'ph'), may hold values from -0.046875 to 0.046875
- tile_rows: int32 [8, 16, 128], P('el', 'ph'), may hold values from 0 to 15, as said below
- tile_cols: int32 [8, 16, 128], P('el', 'ph'), may hold values from 0 to 23, as said below
- tile_count: int32 [8, 16], P('el', 'ph'), may hold values from 16 to 128, as said below
Outputs:
- elec_out: float32 [128, 96, 256], P(('el', 'ph'))
- phon_out: float32 [16, 24, 96, 256], P('ph', 'el')
The draws below stay inside these ranges and needn't reach their ends.
Inputs may be any that keep to these rules, and one draw needn't show every extreme that they name: `tile_rows`: block of each slot's tile among the 16 electron blocks of its pattern row; the slots of one cell name distinct (row, column) pairs. `tile_cols`: block of each slot's tile among the 24 phonon blocks of its pattern column. Slots 0 to tile_count - 1 of a cell are live; some cell is full in every draw.
All inputs are finite; a program needn't handle non-finite values.
Results may differ from the reference program's by a relative error of at most 0.0021.
Values may be sent and summed in bfloat16 or wider, within the bound.
A program may use at most 128 MiB of HBM per device.

```python
import math
import jax
import jax.numpy as jnp
from jax import lax

TILE = 256
EBLOCKS = 128
PBLOCKS = 384
TILES_DEV = 128
ITERS = 3
RHS = 96
ERB = 16
PCOL = 24
N_EL = 8
N_PH = 16


def pattern(key):
    key = jax.random.fold_in(key, 71)
    col_span = PBLOCKS // N_PH
    cell_total = EBLOCKS // N_EL * col_span
    keys = jax.random.split(key, N_EL * N_PH)
    picks = jax.vmap(lambda single: jax.random.permutation(single, cell_total)[:TILES_DEV])(keys)
    picks = picks.reshape(N_EL, N_PH, TILES_DEV).astype(jnp.int32)
    return (picks // col_span, picks % col_span)


def draw_tile_rows(key, part):
    return pattern(key)[0]


def draw_tile_cols(key, part):
    return pattern(key)[1]


def draw_tile_count(key, part):
    key = jax.random.fold_in(key, 113)
    first_key, second_key = jax.random.split(key)
    units = jax.random.randint(first_key, (N_EL * N_PH,), 0, 33).astype(jnp.int32)
    lowest = TILES_DEV // 8
    counts = lowest + (TILES_DEV - lowest) * units * units * units // 32768
    chosen = jax.random.randint(second_key, (), 0, N_EL * N_PH).astype(jnp.int32)
    counts = jnp.where(jnp.arange(N_EL * N_PH, dtype=jnp.int32) == chosen, TILES_DEV, counts)
    return counts.astype(jnp.int32).reshape(N_EL, N_PH)


def steps_of(own_key, dims, shards, least, largest):
    factor_of, own = 1.0, jax.random.fold_in(own_key, 6)
    for position, blocks in shards:
        steps = jnp.exp(jax.random.uniform(jax.random.fold_in(own, position), (blocks,), jnp.float32, least / len(shards), largest / len(shards)))
        factor_of = factor_of * jnp.repeat(steps, dims[position] // blocks).reshape([-1 if axis == position else 1 for axis in range(len(dims))])
    return factor_of


def bell_draw(stream_key, shape, spread, reach, cuts=(), kind=jnp.bfloat16):
    factor_of = steps_of(stream_key, shape, cuts, -0.22, 0.18) if cuts else 1.0
    values = jax.random.normal(stream_key, shape, jnp.float32) * spread * factor_of
    return jnp.minimum(jnp.maximum(values, -reach), reach).astype(kind)


def setup_inputs(seed: int = 0) -> dict:
    arg_keys = jax.random.split(jax.random.key(seed), 11)
    elec_dev = bell_draw(arg_keys[0], (EBLOCKS, RHS, TILE), 1.0, 6.0, ((0, 128),), jnp.float32)
    phon_dev = bell_draw(arg_keys[1], (N_PH, PCOL, RHS, TILE), 1.0, 6.0, ((0, 16), (1, 8)), jnp.float32)
    elec_source = bell_draw(arg_keys[2], (EBLOCKS, RHS, TILE), 1.0, 6.0, ((0, 128),), jnp.float32)
    phon_source = bell_draw(arg_keys[3], (N_PH, PCOL, RHS, TILE), 1.0, 6.0, ((0, 16), (1, 8)), jnp.float32)
    elec_rate = jnp.clip(jnp.exp(math.log(3.0) - 1.3862944 * jax.random.uniform(arg_keys[4], (EBLOCKS, TILE), jnp.float32) ** steps_of(arg_keys[4], (EBLOCKS, TILE), ((0, 128),), -0.2, 0.2)), 0.75, 3.0)
    phon_rate = jnp.clip(jnp.exp(math.log(3.0) - 1.3862944 * jax.random.uniform(arg_keys[5], (N_PH, PCOL, TILE), jnp.float32) ** steps_of(arg_keys[5], (N_PH, PCOL, TILE), ((0, 16), (1, 8)), -0.2, 0.2)), 0.75, 3.0)
    tiles = bell_draw(arg_keys[6], (N_EL, N_PH, TILES_DEV, TILE, TILE), (TILE * TILES_DEV * N_PH // (2 * ERB)) ** -0.5, 0.046875, ((0, 8), (1, 16)))
    tile_rows = draw_tile_rows(jax.random.fold_in(arg_keys[10], 71), 0)
    tile_cols = draw_tile_cols(jax.random.fold_in(arg_keys[10], 71), 0)
    tile_count = draw_tile_count(jax.random.fold_in(arg_keys[10], 71), 0)
    return dict(elec_dev=elec_dev, phon_dev=phon_dev, elec_source=elec_source, phon_source=phon_source, elec_rate=elec_rate, phon_rate=phon_rate, tiles=tiles, tile_rows=tile_rows, tile_cols=tile_cols, tile_count=tile_count)


def reference(elec_dev, phon_dev, elec_source, phon_source, elec_rate, phon_rate, tiles, tile_rows, tile_cols, tile_count):
    row_span = EBLOCKS // N_EL
    col_span = PBLOCKS // N_PH
    cell_count = N_EL * N_PH
    row_base = (jnp.arange(N_EL, dtype=jnp.int32) * row_span)[:, None, None]
    col_base = (jnp.arange(N_PH, dtype=jnp.int32) * col_span)[None, :, None]
    global_rows = (tile_rows + row_base).astype(jnp.int32).reshape(cell_count, TILES_DEV)
    global_cols = (tile_cols + col_base).astype(jnp.int32).reshape(cell_count, TILES_DEV)
    slot_index = jnp.arange(TILES_DEV, dtype=jnp.int32)
    active = (slot_index[None, None, :] < tile_count[:, :, None]).reshape(cell_count, TILES_DEV)
    tile_sets = tiles.reshape(cell_count, TILES_DEV, TILE, TILE)
    elec = elec_dev
    phon = phon_dev.reshape(PBLOCKS, RHS, TILE)
    phon_src = phon_source.reshape(PBLOCKS, RHS, TILE)
    elec_scale = elec_rate[:, None, :]
    phon_scale = phon_rate.reshape(PBLOCKS, TILE)[:, None, :]
    for sweep_index in range(ITERS):
        elec_half = elec.astype(jnp.bfloat16)
        phon_half = phon.astype(jnp.bfloat16)

        def one_cell(totals, inputs):
            elec_total, phon_total = totals
            tile_set, row_ids, col_ids, slot_flags = inputs
            weights = tile_set.astype(jnp.float32)
            elec_in = elec_half[row_ids].astype(jnp.float32)
            phon_in = phon_half[col_ids].astype(jnp.float32)
            slot_mask = jnp.where(slot_flags, 1.0, 0.0).astype(jnp.float32)[:, None, None]
            to_phonon = jnp.einsum("tka,tab->tkb", elec_in, weights, precision=lax.Precision.HIGHEST) * slot_mask
            to_electron = jnp.einsum("tkb,tab->tka", phon_in, weights, precision=lax.Precision.HIGHEST) * slot_mask
            return (elec_total.at[row_ids].add(to_electron), phon_total.at[col_ids].add(to_phonon)), None

        zero_totals = (jnp.zeros((EBLOCKS, RHS, TILE), jnp.float32), jnp.zeros((PBLOCKS, RHS, TILE), jnp.float32))
        drags, unused = lax.scan(one_cell, zero_totals, (tile_sets, global_rows, global_cols, active))
        elec = (elec_source + drags[0]) / elec_scale
        phon = (phon_src + drags[1]) / phon_scale
    return elec, phon.reshape(N_PH, col_span, RHS, TILE)
```

```python
import jax
import jax.numpy as jnp
from jax import lax
from jax.experimental import pallas as pl
from jax.experimental.pallas import tpu as pltpu
from jax.sharding import Mesh
from jax.sharding import PartitionSpec as P

ITERS = 3
EL = ("el_0", "el_1")
EL_PH = ("el_0", "el_1", "ph")
UNROLL = 8
LOADS = 8


def copy_for_each(shard, axis):
    copies = jnp.broadcast_to(shard, (lax.axis_size(axis), *shard.shape))
    return lax.all_to_all(copies, axis, split_axis=0, concat_axis=0, tiled=True)


def gather_directly(shard, axis):
    blocks = copy_for_each(shard, axis)
    return blocks.reshape(-1, *shard.shape[1:])


def summed_on_arrival(shard, axis):
    size = lax.axis_size(axis)
    pieces = shard.reshape(size, -1, *shard.shape[1:])
    arrived = lax.all_to_all(pieces, axis, split_axis=0, concat_axis=0, tiled=True)
    return arrived.sum(axis=0)


def by_block(own, other, live_count, blocks):
    slots = own.shape[0]
    places = jnp.arange(slots, dtype=jnp.int32)
    live = places < live_count
    key = jnp.where(live, own, blocks) * slots + places
    rank = jnp.sum((key[None, :] < key[:, None]).astype(jnp.int32), axis=1)
    chosen = rank[None, :] == places[:, None]

    def sorted_as(values):
        return jnp.sum(jnp.where(chosen, values[None, :], 0), axis=1)

    order = sorted_as(places)
    partner = sorted_as(jnp.where(live, other, 0))
    block = sorted_as(jnp.where(live, own, blocks))
    before = jnp.concatenate([jnp.full((1,), -1, jnp.int32), block[:-1]])
    keep = (block == before).astype(jnp.float32)
    ids = jnp.arange(blocks, dtype=jnp.int32)
    up_to = jnp.sum(((own[None, :] <= ids[:, None]) & live[None, :]).astype(jnp.int32), axis=1)
    own_number = jnp.sum(((own[None, :] == ids[:, None]) & live[None, :]).astype(jnp.int32), axis=1)
    return order, partner, keep, jnp.maximum(up_to - 1, 0), jnp.minimum(own_number, 1).astype(jnp.float32)


def pass_kernel(
    p_order, p_other, p_keep, p_last, p_any, e_order, e_other, e_keep, e_last, e_any,
    tiles_hbm, elec, phon, elec_drag, phon_drag, tiles, partial, sems,
):
    slots = tiles.shape[0]
    part = slots // LOADS
    copies = [
        pltpu.make_async_copy(tiles_hbm.at[pl.ds(part * i, part)], tiles.at[pl.ds(part * i, part)], sems.at[i])
        for i in range(LOADS)
    ]
    for copy in copies:
        copy.start()
    for copy in copies:
        copy.wait()

    def run(order, other, keep, source, contract):
        def steps(group, total):
            for step in range(UNROLL):
                place = group * UNROLL + step
                product = lax.dot_general(
                    source[other[place]],
                    tiles[order[place]],
                    (((1,), (contract,)), ((), ())),
                    preferred_element_type=jnp.float32,
                )
                total = total * keep[place] + product
                partial[place] = total
            return total

        lax.fori_loop(0, slots // UNROLL, steps, jnp.zeros(partial.shape[1:], jnp.float32))

    run(p_order, p_other, p_keep, elec, 0)
    for block in range(phon_drag.shape[0]):
        phon_drag[block] = partial[p_last[block]] * p_any[block]
    run(e_order, e_other, e_keep, phon, 1)
    for block in range(elec_drag.shape[0]):
        elec_drag[block] = partial[e_last[block]] * e_any[block]


def tile_pass(tables, tile_set, elec_blocks, phon_blocks):
    vmem = pl.BlockSpec(memory_space=pltpu.VMEM)
    slots, side, _ = tile_set.shape
    rhs = elec_blocks.shape[1]
    return pl.pallas_call(
        pass_kernel,
        out_shape=(
            jax.ShapeDtypeStruct(elec_blocks.shape, jnp.float32),
            jax.ShapeDtypeStruct(phon_blocks.shape, jnp.float32),
        ),
        in_specs=[pl.BlockSpec(memory_space=pltpu.SMEM)] * 10
        + [pl.BlockSpec(memory_space=pl.ANY), vmem, vmem],
        out_specs=(vmem, vmem),
        scratch_shapes=[
            pltpu.VMEM((slots, side, side), jnp.bfloat16),
            pltpu.VMEM((slots, rhs, side), jnp.float32),
            pltpu.SemaphoreType.DMA((LOADS,)),
        ],
        compiler_params=pltpu.CompilerParams(vmem_limit_bytes=44 * 2**20),
        cost_estimate=pl.CostEstimate(
            flops=4 * slots * rhs * side * side, bytes_accessed=2 * slots * side * side, transcendentals=0
        ),
        name="tile_pass",
    )(*tables, tile_set, elec_blocks, phon_blocks)


def local(
    elec_dev, phon_dev, elec_source, phon_source, elec_rate, phon_rate, tiles, tile_rows, tile_cols, tile_count
):
    rows, cols, count = tile_rows[0, 0], tile_cols[0, 0], tile_count[0, 0]
    elec_range = gather_directly(elec_dev.astype(jnp.bfloat16), "ph")
    phon_range = gather_directly(phon_dev[0].astype(jnp.bfloat16), EL)
    tables = by_block(cols, rows, count, phon_range.shape[0]) + by_block(rows, cols, count, elec_range.shape[0])
    elec_now, phon_now = elec_dev, phon_dev[0]
    for sweep in range(ITERS):
        elec_drag, phon_drag = tile_pass(tables, tiles[0, 0], elec_range, phon_range)
        elec_now = (elec_source + summed_on_arrival(elec_drag, "ph")) / elec_rate[:, None, :]
        phon_now = (phon_source[0] + summed_on_arrival(phon_drag, EL)) / phon_rate[0][:, None, :]
        if sweep + 1 < ITERS:
            elec_range = gather_directly(elec_now.astype(jnp.bfloat16), "ph")
            phon_range = gather_directly(phon_now.astype(jnp.bfloat16), EL)
    return elec_now, phon_now[None]


def solution(mesh):
    split = Mesh(mesh.devices.reshape(4, 2, mesh.shape["ph"]), EL_PH)
    placed = (
        P(EL_PH, None, None),
        P("ph", EL, None, None),
        P(EL_PH, None, None),
        P("ph", EL, None, None),
        P(EL_PH, None),
        P("ph", EL, None),
        P(EL, "ph", None, None, None),
        P(EL, "ph", None),
        P(EL, "ph", None),
        P(EL, "ph"),
    )
    return jax.shard_map(
        local,
        mesh=split,
        in_specs=placed,
        out_specs=(P(EL_PH, None, None), P("ph", EL, None, None)),
        check_vma=False,
    )
```

```python
import jax
import jax.numpy as jnp
from jax import lax
from jax.experimental import pallas as pl
from jax.experimental.pallas import tpu as pltpu
from jax.sharding import PartitionSpec as P

ITERS = 3
UNROLL = 8
LOADS = 8
TOP = 32000.0
FINE = 8.0
MESH = pl.DeviceIdType.MESH


def by_block(own, other, live_count, blocks):
    slots = own.shape[0]
    places = jnp.arange(slots, dtype=jnp.int32)
    live = places < live_count
    key = jnp.where(live, own, blocks) * slots + places
    rank = jnp.sum((key[None, :] < key[:, None]).astype(jnp.int32), axis=1)
    chosen = rank[None, :] == places[:, None]

    def sorted_as(values):
        return jnp.sum(jnp.where(chosen, values[None, :], 0), axis=1)

    order = sorted_as(places)
    partner = sorted_as(jnp.where(live, other, 0))
    block = sorted_as(jnp.where(live, own, blocks))
    before = jnp.concatenate([jnp.full((1,), -1, jnp.int32), block[:-1]])
    keep = (block == before).astype(jnp.float32)
    ids = jnp.arange(blocks, dtype=jnp.int32)
    up_to = jnp.sum(((own[None, :] <= ids[:, None]) & live[None, :]).astype(jnp.int32), axis=1)
    own_number = jnp.sum(((own[None, :] == ids[:, None]) & live[None, :]).astype(jnp.int32), axis=1)
    return order, partner, keep, jnp.maximum(up_to - 1, 0), jnp.minimum(own_number, 1).astype(jnp.float32)


(AX, AYP, AYM, AHP, AHM, AQP, AQM, AOX) = range(8)
(R8, R6, R7, R4, R5, R1, R2, R3) = range(8, 16)
GE = 16
SE = 31
MESSAGES = 39


def kernel(
    p_order, p_other, p_keep, p_last, p_any, e_order, e_other, e_keep, e_last, e_any,
    tiles_hbm, elec_dev, phon_dev, elec_source, phon_source, elec_rate, phon_rate,
    elec_out, phon_out,
    tiles, seg_p, seg_e, pb, eb, psend, precv, dsend, drecv, esend, erecv, tmp,
    load_sems, send_sems, recv_sems,
):
    slots = tiles.shape[0]
    part = slots // LOADS
    loads = [
        pltpu.make_async_copy(tiles_hbm.at[pl.ds(part * i, part)], tiles.at[pl.ds(part * i, part)], load_sems.at[i])
        for i in range(LOADS)
    ]
    for load in loads:
        load.start()

    el, ph = lax.axis_index("el"), lax.axis_index("ph")
    y, xl = lax.div(el, 2), lax.rem(el, 2)
    yp, ym, yo, xq = lax.rem(y + 1, 4), lax.rem(y + 3, 4), lax.rem(y + 2, 4), 1 - xl
    xh, z, core = lax.div(ph, 8), lax.rem(lax.div(ph, 2), 4), lax.rem(ph, 2)
    zp, zm, zo, hq = lax.rem(z + 1, 4), lax.rem(z + 3, 4), lax.rem(z + 2, 4), 1 - xh

    def at_y(yy, xx):
        return 2 * yy + xx

    def at_z(hh, zz, cc):
        return 8 * hh + 2 * zz + cc

    p_x, p_yp, p_ym = (at_y(y, xq), ph), (at_y(yp, xl), ph), (at_y(ym, xl), ph)
    sib = (el, at_z(xh, z, 1 - core))
    e_zp, e_zm, e_zo, e_x = (
        (el, at_z(xh, zp, core)),
        (el, at_z(xh, zm, core)),
        (el, at_z(xh, zo, core)),
        (el, at_z(hq, z, core)),
    )

    barrier = pltpu.get_barrier_semaphore()
    for peer in (p_x, p_yp, p_ym, sib, e_zp, e_zm, e_zo, e_x):
        pl.semaphore_signal(barrier, inc=1, device_id=peer, device_id_type=MESH)
    pl.semaphore_wait(barrier, 8)

    def message(s, i, src, dst, peer):
        return pltpu.make_async_remote_copy(
            src_ref=src,
            dst_ref=dst,
            send_sem=send_sems.at[s, i],
            recv_sem=recv_sems.at[s, i],
            device_id=peer,
            device_id_type=MESH,
        )

    def unit(s, yy, xx):
        return pb.at[s, pl.ds(3 * at_y(yy, xx), 3)]

    def half(s, yy, xx, h):
        return pb.at[s, pl.ds(3 * at_y(yy, xx), 3), pl.ds(48 * h, 48)]

    def gather_p(s):
        def pair(i, peer, sent, got):
            return (lambda: message(s, i, sent, sent, peer)), (lambda: message(s, i, got, got, peer))

        return {
            AX: pair(AX, p_x, unit(s, y, xl), unit(s, y, xq)),
            AYP: pair(AYP, p_yp, unit(s, y, xl), unit(s, ym, xl)),
            AYM: pair(AYM, p_ym, unit(s, y, xl), unit(s, yp, xl)),
            AHP: pair(AHP, p_yp, half(s, ym, xl, 0), half(s, yo, xl, 0)),
            AHM: pair(AHM, p_ym, half(s, yp, xl, 1), half(s, yo, xl, 1)),
            AQP: pair(AQP, p_yp, unit(s, y, xq), unit(s, ym, xq)),
            AQM: pair(AQM, p_ym, unit(s, y, xq), unit(s, yp, xq)),
            AOX: pair(AOX, p_x, unit(s, yo, xl), unit(s, yo, xq)),
        }

    def eblock(s, hh, zz, cc):
        return eb.at[s, at_z(hh, zz, cc)]

    def gather_e(s):
        def pair(i, peer, sent, got):
            return (lambda: message(s, i, sent, sent, peer)), (lambda: message(s, i, got, got, peer))

        out = {}
        for k, (peer, came) in enumerate(((e_x, None), (e_zp, zm), (e_zm, zp), (e_zo, zo))):
            if came is None:
                out[k] = pair(GE + k, peer, eblock(s, xh, z, core), eblock(s, hq, z, core))
            else:
                out[k] = pair(GE + k, peer, eblock(s, xh, z, core), eblock(s, xh, came, core))
                out[k + 3] = pair(GE + k + 3, peer, eblock(s, hq, z, core), eblock(s, hq, came, core))
        for k, (hh, zz) in enumerate(
            ((xh, z), (hq, z), (xh, zm), (xh, zp), (xh, zo), (hq, zm), (hq, zp), (hq, zo))
        ):
            out[7 + k] = pair(GE + 7 + k, sib, eblock(s, hh, zz, core), eblock(s, hh, zz, 1 - core))
        return out

    def send(table, *ids):
        for i in ids:
            table[i][0]().start()

    def got(table, *ids):
        for i in ids:
            table[i][1]().wait_recv()

    def sent(table):
        for out, _ in table.values():
            out().wait_send()

    def start_gather_p(s):
        send(gather_p(s), AX, AYP, AYM)

    def start_gather_e(s):
        send(gather_e(s), 0, 1, 2, 3, 7)

    def finish_gathers(s):
        p, e = gather_p(s), gather_e(s)
        got(e, 0)
        send(e, 4, 5, 6, 8)
        got(e, 1, 2)
        send(e, 9, 10)
        got(p, AYP)
        send(p, AHP)
        got(p, AYM)
        send(p, AHM)
        got(p, AX)
        send(p, AQP, AQM)
        got(e, 3)
        send(e, 11)
        got(e, 4, 5)
        send(e, 12, 13)
        got(e, 6)
        send(e, 14)
        got(p, AHP, AHM)
        send(p, AOX)
        got(e, 7, 8, 9, 10, 11, 12, 13, 14)
        got(p, AQP, AQM, AOX)
        sent(e)
        sent(p)

    def run(order, other, keep, source, contract, partial):
        def steps(group, total):
            for step in range(UNROLL):
                place = group * UNROLL + step
                product = lax.dot_general(
                    source[other[place]],
                    tiles[order[place]],
                    (((1,), (contract,)), ((), ())),
                    preferred_element_type=jnp.float32,
                )
                total = total * keep[place] + product
                partial[place] = total
            return total

        lax.fori_loop(0, slots // UNROLL, steps, jnp.zeros(partial.shape[1:], jnp.float32))

    def own_p(u):
        def value(i, k):
            block = 3 * u + lax.div(i, 2)
            rows = pl.ds(pl.multiple_of(48 * lax.rem(i, 2) + 16 * k, 16), 16)
            return seg_p[p_last[block], rows, :] * p_any[block]

        return value

    def own_e(block):
        def value(i, k):
            rows = pl.ds(pl.multiple_of(48 * i + 16 * k, 16), 16)
            return seg_e[e_last[block], rows, :] * e_any[block]

        return value

    def scale_of(ref, scale_row):
        coded = ref[scale_row : scale_row + 16, :].astype(jnp.int32).astype(jnp.float32)
        return jnp.exp2(coded * (1.0 / FINE)) * (1.0 / TOP)

    def over(pieces, carry, own, scale_row, extra, visit):
        for shift, first, end, refs in pieces:
            scales = [scale_of(ref, scale_row) for ref in refs]

            def body(i, carry, shift=shift, refs=refs, scales=scales):
                for k in range(3):
                    row = pl.multiple_of(48 * i + 16 * k, 16)
                    value = own(i, k)
                    if extra is not None:
                        value = value + extra(i, k)
                    for ref, scale in zip(refs, scales):
                        coded = ref[pl.ds(pl.multiple_of(row + shift, 16), 16), :]
                        value = value + coded.astype(jnp.int32).astype(jnp.float32) * scale
                    carry = visit(row, i, k, value, carry)
                return carry

            carry = lax.fori_loop(first, end, body, carry)
        return carry

    def code(out, pieces, own, scale_row, extra=None):
        def keep_it(row, i, k, value, most):
            tmp[pl.ds(row, 16), :] = value
            return jnp.maximum(most, jnp.abs(value))

        most = over(pieces, jnp.zeros((16, tmp.shape[1]), jnp.float32), own, scale_row, extra, keep_it)
        level = jnp.ceil(jnp.log2(jnp.maximum(most, 1e-30)) * FINE)
        out[scale_row : scale_row + 16, :] = level.astype(jnp.int32).astype(jnp.int16)
        scale = jnp.exp2(level * (-1.0 / FINE)) * TOP
        for shift, first, end, _ in pieces:

            def body(i, carry, shift=shift):
                for k in range(3):
                    row = pl.multiple_of(48 * i + 16 * k, 16)
                    whole = jnp.round(tmp[pl.ds(row, 16), :] * scale).astype(jnp.int32)
                    out[pl.ds(pl.multiple_of(row + shift, 16), 16), :] = whole.astype(jnp.int16)
                return carry

            lax.fori_loop(first, end, body, 0)

    def code_p(slot, u, low=(), high=()):
        code(psend.at[slot], ((0, 0, 3, low), (16, 3, 6, high)), own_p(u), 144)

    def pair_e(s, hh, zz):
        value = own_e(at_z(hh, zz, core))
        k4 = 4 * hh + zz

        def both(i, k):
            rows = pl.ds(pl.multiple_of(48 * i + 16 * k, 16), 16)
            return value(i, k) + drecv[s, k4, rows, :]

        return both

    def code_e(s, slot, hh, zz, refs=()):
        code(esend.at[slot], ((0, 0, 2, refs),), pair_e(s, hh, zz), 96)

    pb[0, pl.ds(3 * el, 3)] = phon_dev[...].astype(jnp.bfloat16)
    start_gather_p(0)
    eb[0, ph] = elec_dev[...].astype(jnp.bfloat16)
    start_gather_e(0)
    finish_gathers(0)
    for load in loads:
        load.wait()

    def sweep(s, _):
        run(p_order, p_other, p_keep, eb.at[s], 0, seg_p)

        rp = {}

        def route(i, peer, src, dst):
            rp[i] = (lambda: message(s, i, src, dst, peer),) * 2

        route(R8, p_x, psend.at[0], precv.at[s, 0])
        route(R6, p_ym, psend.at[1], precv.at[s, 1])
        route(R7, p_yp, psend.at[2], precv.at[s, 2])
        route(R4, p_ym, psend.at[3, pl.ds(0, 160)], precv.at[s, 3, pl.ds(0, 160)])
        route(R5, p_yp, psend.at[3, pl.ds(144, 160)], precv.at[s, 7, pl.ds(144, 160)])
        route(R1, p_x, psend.at[4], precv.at[s, 4])
        route(R2, p_ym, psend.at[5], precv.at[s, 5])
        route(R3, p_yp, psend.at[6], precv.at[s, 6])

        re = {}

        def route_e(i, peer, src, dst):
            re[i] = (lambda: message(s, SE + i, src, dst, peer),) * 2

        route_e(7, sib, dsend, drecv.at[s])
        for i, peer in enumerate((e_zp, e_zm, e_zo, e_zp, e_zm, e_zo, e_x)):
            route_e(i, peer, esend.at[i], erecv.at[s, i])

        code_p(0, at_y(yo, xq))
        send(rp, R8)
        code_p(1, at_y(ym, xq))
        send(rp, R6)
        code_p(2, at_y(yp, xq))
        send(rp, R7)

        run(e_order, e_other, e_keep, pb.at[s], 1, seg_e)

        for k in range(8):
            block = at_z(k // 4, k % 4, 1 - core)
            dsend[k] = seg_e[e_last[block]] * e_any[block]
        send(re, 7)

        got(rp, R8)
        code_p(3, at_y(yo, xl), (precv.at[s, 0],), (precv.at[s, 0],))
        send(rp, R4, R5)
        got(rp, R6, R7)
        code_p(4, at_y(y, xq), (precv.at[s, 1], precv.at[s, 2]), (precv.at[s, 1], precv.at[s, 2]))
        send(rp, R1)

        got(re, 7)
        for i, (hh, zz) in enumerate(((hq, zp), (hq, zm), (hq, zo), (xh, zp), (xh, zm), (xh, zo))):
            code_e(s, i, hh, zz)
            send(re, i)

        got(rp, R4)
        code_p(5, at_y(ym, xl), (precv.at[s, 3],), ())
        send(rp, R2)
        got(rp, R5)
        code_p(6, at_y(yp, xl), (), (precv.at[s, 7],))
        send(rp, R3)

        got(re, 0, 1, 2)
        code_e(s, 6, hq, z, (erecv.at[s, 0], erecv.at[s, 1], erecv.at[s, 2]))
        send(re, 6)
        got(re, 3, 4, 5)

        got(rp, R1, R2, R3)
        arrived = tuple(precv.at[s, i] for i in (4, 5, 6))

        def new_p(row, i, k, value, carry):
            third = lax.div(i, 2)
            rows = pl.ds(pl.multiple_of(48 * lax.rem(i, 2) + 16 * k, 16), 16)
            phon_out[third, rows, :] = (phon_source[third, rows, :] + value) / phon_rate[third]
            return carry

        over(((0, 0, 3, arrived), (16, 3, 6, arrived)), 0, own_p(el), 144, None, new_p)

        @pl.when(s < ITERS - 1)
        def _():
            pb[s + 1, pl.ds(3 * el, 3)] = phon_out[...].astype(jnp.bfloat16)
            start_gather_p(s + 1)

        got(re, 6)
        arrived_e = tuple(erecv.at[s, i] for i in (3, 4, 5, 6))

        def new_e(row, i, k, value, carry):
            rows = pl.ds(row, 16)
            elec_out[rows, :] = (elec_source[rows, :] + value) / elec_rate[...]
            return carry

        over(((0, 0, 2, arrived_e),), 0, pair_e(s, xh, z), 96, None, new_e)
        sent(rp)
        sent(re)

        @pl.when(s < ITERS - 1)
        def _():
            eb[s + 1, ph] = elec_out[...].astype(jnp.bfloat16)
            start_gather_e(s + 1)
            finish_gathers(s + 1)

        return 0

    lax.fori_loop(0, ITERS, sweep, 0)


def local(
    elec_dev, phon_dev, elec_source, phon_source, elec_rate, phon_rate, tiles, tile_rows, tile_cols, tile_count
):
    rows, cols, count = tile_rows[0, 0], tile_cols[0, 0], tile_count[0, 0]
    tables = by_block(cols, rows, count, 24) + by_block(rows, cols, count, 16)
    slots, side, _ = tiles.shape[2:]
    rhs = elec_dev.shape[1]
    vmem = pl.BlockSpec(memory_space=pltpu.VMEM)
    elec_out, phon_out = pl.pallas_call(
        kernel,
        out_shape=(
            jax.ShapeDtypeStruct((rhs, side), jnp.float32),
            jax.ShapeDtypeStruct((3, rhs, side), jnp.float32),
        ),
        in_specs=[pl.BlockSpec(memory_space=pltpu.SMEM)] * 10 + [pl.BlockSpec(memory_space=pl.ANY)] + [vmem] * 6,
        out_specs=(vmem, vmem),
        scratch_shapes=[
            pltpu.VMEM((slots, side, side), jnp.bfloat16),
            pltpu.VMEM((slots, rhs, side), jnp.float32),
            pltpu.VMEM((slots, rhs, side), jnp.float32),
            pltpu.VMEM((ITERS, 24, rhs, side), jnp.bfloat16),
            pltpu.VMEM((ITERS, 16, rhs, side), jnp.bfloat16),
            pltpu.VMEM((7, 304, side), jnp.int16),
            pltpu.VMEM((ITERS, 8, 304, side), jnp.int16),
            pltpu.VMEM((8, rhs, side), jnp.float32),
            pltpu.VMEM((ITERS, 8, rhs, side), jnp.float32),
            pltpu.VMEM((7, 112, side), jnp.int16),
            pltpu.VMEM((ITERS, 7, 112, side), jnp.int16),
            pltpu.VMEM((288, side), jnp.float32),
            pltpu.SemaphoreType.DMA((LOADS,)),
            pltpu.SemaphoreType.DMA((ITERS, MESSAGES)),
            pltpu.SemaphoreType.DMA((ITERS, MESSAGES)),
        ],
        compiler_params=pltpu.CompilerParams(
            vmem_limit_bytes=62 * 2**20, collective_id=0, has_side_effects=True
        ),
        name="sweeps",
    )(
        *tables,
        tiles[0, 0],
        elec_dev[0],
        phon_dev[0],
        elec_source[0],
        phon_source[0],
        elec_rate,
        phon_rate[0][:, None, :],
    )
    return elec_out[None], phon_out[None]


def solution(mesh):
    both = ("el", "ph")
    placed = (
        P(both, None, None),
        P("ph", "el", None, None),
        P(both, None, None),
        P("ph", "el", None, None),
        P(both, None),
        P("ph", "el", None),
        P("el", "ph", None, None, None),
        P("el", "ph", None),
        P("el", "ph", None),
        P("el", "ph"),
    )
    return jax.shard_map(
        local,
        mesh=mesh,
        in_specs=placed,
        out_specs=(P(both, None, None), P("ph", "el", None, None)),
        check_vma=False,
    )
```

```python
import random

import jax
import jax.numpy as jnp
from jax import lax
from jax.experimental import pallas as pl
from jax.experimental.pallas import tpu as pltpu
from jax.sharding import PartitionSpec as P

ITERS = 3
UNROLL = 8
LOADS = 8
PIECES = 5
TOP = 32000.0
FINE = 8.0
MESH = pl.DeviceIdType.MESH

WIRE = 46.7e3
HOP = {"x": 1.9, "y+": 2.0, "y-": 2.0, "z+": 2.0, "z-": 2.0, "zz": 2.5, "xx": 2.5, "d": 0.9}
LINK = {"x": "x", "xx": "x", "y+": "y+", "y-": "y-", "z+": "z+", "z-": "z-", "zz": "z+", "d": "d"}
LOAD = {"xx": 1.2, "zz": 1.2, "d": 0.07}
PASSES = (("P", 0), ("E", 0), ("E", 1), ("P", 1), ("P", 2), ("E", 2))
SEED = 0
SPREAD = 0.0
P_HALF, P_CODED, E_BLOCK, E_CODED = 3 * 48 * 512, 160 * 512, 96 * 512, 112 * 512


class Plan:
    def __init__(self):
        self.steps = {}

    def add(self, name, cost, after=(), needs=(), sends=()):
        self.steps[name] = (cost, tuple(after), tuple(needs), tuple(sends))

    def order(self):
        chance = random.Random(SEED)
        lean = {n: chance.uniform(1.0 - SPREAD, 1.0 + SPREAD) for n in self.steps}
        sender = {m: (n, way, size) for n, (_, _, _, sends) in self.steps.items() for m, way, size in sends}
        users = {n: [] for n in self.steps}
        for name, (_, after, needs, _) in self.steps.items():
            for n in after:
                users[n].append((name, 0.0))
            for m in needs:
                n, way, size = sender[m]
                users[n].append((name, HOP[way] + size * LOAD.get(way, 1.0) / WIRE))
        tail = {}

        def rest(name):
            if name not in tail:
                cost = self.steps[name][0]
                tail[name] = cost + max((gap + rest(n) for n, gap in users[name]), default=0.0)
            return tail[name]

        now, free, arrival, done, result = 0.0, {}, {}, set(), []
        left = dict.fromkeys(self.steps)
        while left:
            ready = []
            for name in left:
                _, after, needs, _ = self.steps[name]
                if all(n in done for n in after) and all(m in arrival for m in needs):
                    urgent = 1000.0 if self.steps[name][0] < 0.04 else 0.0
                    ready.append((max([now] + [arrival[m] for m in needs]), -rest(name) * lean[name] - urgent, name))
            soonest = min(ready)[0]
            start, _, name = min((r for r in ready if r[0] <= max(now, soonest) + 0.05), key=lambda r: r[1])
            cost, _, _, sends = self.steps[name]
            now = start + cost
            for m, way, size in sends:
                link = LINK[way]
                begin = max(now, free.get(link, 0.0))
                free[link] = begin + size * LOAD.get(way, 1.0) / WIRE
                arrival[m] = free[link] + HOP[way]
            done.add(name)
            del left[name]
            result.append((name, start, now))
        return result


def plan():
    p = Plan()
    for s in range(ITERS):
        if s == 0:
            p.add(("put_e", 0), 0.05, (), (), e_first(0))
            for h in range(2):
                p.add(("put_p", 0, h), 0.05, (("put_e", 0),), (), p_first(0, h))
        own_p = [("put_p", s, h) for h in range(2)]
        for m, by, way, h in (("AHP", "AYP", "y+", 0), ("AHM", "AYM", "y-", 1)):
            p.add((m, s), 0.01, (), ((by, s, h),), (((m, s), way, P_HALF),))
        for h, by in ((0, "AHP"), (1, "AHM")):
            p.add(("AQ", s, h), 0.02, (), (("AX", s, h),), ((("AQP", s, h), "y+", P_HALF), (("AQM", s, h), "y-", P_HALF)))
            p.add(("AOX", s, h), 0.01, (), ((by, s),), ((("AOX", s, h), "x", P_HALF),))
        p.add(("F", s), 0.03, (), (("G", s, 0),), e_onward(s))
        for k, by in ((9, 1), (10, 2), (11, 3), (12, 4), (13, 5), (14, 6)):
            p.add(("S", s, k), 0.01, (), (("G", s, by),), ((("G", s, k), "d", E_BLOCK),))
        all_p = [(m, s, h) for m in ("AX", "AYP", "AYM", "AQP", "AQM", "AOX") for h in range(2)]
        all_p += [("AHP", s), ("AHM", s)]
        all_e = [("G", s, k) for k in range(15)]
        for k in range(PIECES):
            for way, arrived, extra in (("P", all_e, [("put_e", s)]), ("E", all_p, own_p)):
                if k:
                    p.add((way, s, k), (P_TIME if way == "P" else E_TIME) / PIECES, ((way, s, k - 1),))
                else:
                    old = [n for n in p.steps if n[1] == s - 1 and n[0] in (P_CODES if way == "P" else E_CODES)]
                    old = [n for n in old if n != ("T", s - 1, 6)]
                    if way == "P" and s:
                        old += own_p
                    p.add((way, s, k), (P_TIME if way == "P" else E_TIME) / PIECES, old + extra, arrived)
        last_p, last_e = (("P", s, PIECES - 1),), (("E", s, PIECES - 1),)
        for h in range(2):
            for m, way in (("R8", "x"), ("R6", "y-"), ("R7", "y+")):
                p.add((m, s, h), 0.13, last_p, (), (((m, s, h), way, P_CODED),))
        p.add(("R4", s, 0), 0.14, last_p, (("R8", s, 0),), ((("R4", s, 0), "y-", P_CODED),))
        p.add(("R5", s, 1), 0.14, last_p, (("R8", s, 1),), ((("R5", s, 1), "y+", P_CODED),))
        for h in range(2):
            p.add(("R1", s, h), 0.15, last_p, (("R6", s, h), ("R7", s, h)), ((("R1", s, h), "x", P_CODED),))
            low, high = ((("R4", s, 0),), ()) if h == 0 else ((), (("R5", s, 1),))
            p.add(("R2", s, h), 0.14, last_p + ((("R4", s, 0),) if h else ()), low, ((("R2", s, h), "y-", P_CODED),))
            p.add(("R3", s, h), 0.14, last_p + (() if h else (("R5", s, 1),)), high, ((("R3", s, h), "y+", P_CODED),))
            p.add(
                ("put_p", s + 1, h), 0.15, last_p, (("R1", s, h), ("R2", s, h), ("R3", s, h)),
                p_first(s + 1, h) if s + 1 < ITERS else (),
            )
        p.add(("D", s), 0.3, last_e, (), ((("D", s), "d", 16 * E_BLOCK),))
        for k, way in enumerate(("z+", "z-", "zz", "z+", "z-", "zz")):
            p.add(("T", s, k), 0.09, last_e, (("D", s),), ((("T", s, k), way, E_CODED),))
        before = (("put_e", s),)
        p.add(("K", s), 0.08, last_e + before, (("D", s),))
        p.add(("T", s, 6), 0.12, (("K", s),), [("T", s, k) for k in range(3)], ((("T", s, 6), "xx", E_CODED),))
        p.add(
            ("put_e", s + 1), 0.15, (("K", s), ("T", s, 6)), [("T", s, k) for k in range(3, 7)],
            e_first(s + 1) if s + 1 < ITERS else (),
        )
    for before, name in zip(PASSES, PASSES[1:]):
        cost, after, needs, sends = p.steps[name + (0,)]
        p.steps[name + (0,)] = (cost, after + (before + (PIECES - 1,),), needs, sends)
    return p


P_TIME, E_TIME = 5.1, 7.5
P_CODES, E_CODES = ("R8", "R6", "R7", "R4", "R5", "R1", "R2", "R3"), ("D", "T", "K")


def e_first(s):
    ways = ("xx", "z+", "z-", "zz")
    return tuple((("G", s, k), way, E_BLOCK) for k, way in enumerate(ways)) + ((("G", s, 7), "d", E_BLOCK),)


def e_onward(s):
    ways = ("z+", "z-", "zz")
    return tuple((("G", s, 4 + k), way, E_BLOCK) for k, way in enumerate(ways)) + ((("G", s, 8), "d", E_BLOCK),)


def p_first(s, h):
    return tuple(((m, s, h), way, P_HALF) for m, way in (("AX", "x"), ("AYP", "y+"), ("AYM", "y-")))


def tables_of(own, other, live, blocks, whole, parts):
    slots = own.shape[1]
    square = (slots, slots)
    here = lax.broadcasted_iota(jnp.int32, square, 1)
    there = lax.broadcasted_iota(jnp.int32, square, 0)

    def down(row):
        return jnp.broadcast_to(row, square).T

    block = jnp.where(live, own, blocks)
    key = block * slots + here[0:1]
    rank = jnp.sum((down(key) < key).astype(jnp.int32), axis=0, keepdims=True)
    place = down(rank)
    block_down = down(block)

    def moved(values, by):
        return jnp.sum(jnp.where(place + by == here, values, 0), axis=0, keepdims=True)

    whole[0:1, :] = moved(there, 0)
    whole[1:2, :] = moved(down(jnp.where(live, other, 0)), 0)
    up_to = jnp.sum((block_down <= here).astype(jnp.int32), axis=0, keepdims=True)
    whole[2:3, :] = jnp.maximum(jnp.where(here[0:1] < blocks, up_to, 1) - 1, 0)
    parts[0:1, :] = (moved(block_down + 1, 0) == moved(block_down + 1, 1)).astype(jnp.float32)
    has = jnp.sum((block_down == here).astype(jnp.int32), axis=0, keepdims=True)
    parts[1:2, :] = (has > 0).astype(jnp.float32)


PER_SWEEP = 51
P_SLOTS = {"R8": 0, "R6": 2, "R7": 4, "R4": 6, "R5": 6, "R1": 8, "R2": 10, "R3": 12}


def kernel(
    count, slot_rows, slot_cols, tiles_hbm, elec_dev, phon_dev, elec_source, phon_source, elec_rate, phon_rate,
    elec_out, phon_out,
    tiles, seg_p, seg_e, pb_0, pb_1, pb_2, eb_0, eb_1, eb_2, psend, precv, dsend, drecv, esend, erecv, kept, tmp,
    whole_v, parts_v, whole, parts, load_sems, table_sems, send_sems, recv_sems,
):
    pb, eb = (pb_0, pb_1, pb_2), (eb_0, eb_1, eb_2)
    slots = tiles.shape[0]
    part = slots // LOADS
    loads = [
        pltpu.make_async_copy(tiles_hbm.at[pl.ds(part * i, part)], tiles.at[pl.ds(part * i, part)], load_sems.at[i])
        for i in range(LOADS)
    ]
    el, ph = lax.axis_index("el"), lax.axis_index("ph")
    y, xl = lax.div(el, 2), lax.rem(el, 2)
    yp, ym, yo, xq = lax.rem(y + 1, 4), lax.rem(y + 3, 4), lax.rem(y + 2, 4), 1 - xl
    xh, z, core = lax.div(ph, 8), lax.rem(lax.div(ph, 2), 4), lax.rem(ph, 2)
    zp, zm, zo, hq = lax.rem(z + 1, 4), lax.rem(z + 3, 4), lax.rem(z + 2, 4), 1 - xh

    def at_y(yy, xx):
        return 2 * yy + xx

    def at_z(hh, zz, cc):
        return 8 * hh + 2 * zz + cc

    p_x, p_yp, p_ym = (at_y(y, xq), ph), (at_y(yp, xl), ph), (at_y(ym, xl), ph)
    sib = (el, at_z(xh, z, 1 - core))
    e_zp, e_zm, e_zo, e_x = (
        (el, at_z(xh, zp, core)),
        (el, at_z(xh, zm, core)),
        (el, at_z(xh, zo, core)),
        (el, at_z(hq, z, core)),
    )

    barrier = pltpu.get_barrier_semaphore()
    for peer in (p_x, p_yp, p_ym, sib, e_zp, e_zm, e_zo, e_x):
        pl.semaphore_signal(barrier, inc=1, device_id=peer, device_id_type=MESH)
    for load in loads:
        load.start()

    live = lax.broadcasted_iota(jnp.int32, (1, slots), 1) < count[0, 0]
    table_copies = []
    for i, (own, other, blocks) in enumerate(((slot_cols, slot_rows, 24), (slot_rows, slot_cols, 16))):
        tables_of(own[...], other[...], live, blocks, whole_v.at[i], parts_v.at[i])
    for i, (src, dst) in enumerate(((whole_v, whole), (parts_v, parts))):
        table_copies.append(pltpu.make_async_copy(src, dst, table_sems.at[i]))
        table_copies[-1].start()
    pl.semaphore_wait(barrier, 8)

    def unit(s, h, yy, xx):
        return pb[s].at[pl.ds(3 * at_y(yy, xx), 3), pl.ds(48 * h, 48)]

    def eblock(s, hh, zz, cc):
        return eb[s].at[at_z(hh, zz, cc)]

    mail = {}

    def route(key, peer, src, dst, got):
        mail[key] = (len(mail), src, dst, peer, got)

    for s in range(ITERS):
        for h in range(2):
            for name, peer, sent, got in (
                ("AX", p_x, (y, xl), (y, xq)),
                ("AYP", p_yp, (y, xl), (ym, xl)),
                ("AYM", p_ym, (y, xl), (yp, xl)),
                ("AQP", p_yp, (y, xq), (ym, xq)),
                ("AQM", p_ym, (y, xq), (yp, xq)),
                ("AOX", p_x, (yo, xl), (yo, xq)),
            ):
                route((name, s, h), peer, unit(s, h, *sent), unit(s, h, *sent), unit(s, h, *got))
            for name, peer in (
                ("R8", p_x), ("R6", p_ym), ("R7", p_yp), ("R1", p_x), ("R2", p_ym), ("R3", p_yp),
                ("R5" if h else "R4", p_yp if h else p_ym),
            ):
                slot = P_SLOTS[name] + h
                route((name, s, h), peer, psend.at[slot], precv.at[s, slot], precv.at[s, slot])
        route(("AHP", s), p_yp, unit(s, 0, ym, xl), unit(s, 0, ym, xl), unit(s, 0, yo, xl))
        route(("AHM", s), p_ym, unit(s, 1, yp, xl), unit(s, 1, yp, xl), unit(s, 1, yo, xl))
        own = eblock(s, xh, z, core)
        far = eblock(s, hq, z, core)
        route(("G", s, 0), e_x, own, own, far)
        for k, (peer, came) in enumerate(((e_zp, zm), (e_zm, zp), (e_zo, zo))):
            route(("G", s, 1 + k), peer, own, own, eblock(s, xh, came, core))
            route(("G", s, 4 + k), peer, far, far, eblock(s, hq, came, core))
        for k, at in enumerate(((xh, z), (hq, z), (xh, zm), (xh, zp), (xh, zo), (hq, zm), (hq, zp), (hq, zo))):
            route(("G", s, 7 + k), sib, eblock(s, *at, core), eblock(s, *at, core), eblock(s, *at, 1 - core))
        route(("D", s), sib, dsend, drecv.at[s], drecv.at[s])
        for k, peer in enumerate((e_zp, e_zm, e_zo, e_zp, e_zm, e_zo, e_x)):
            route(("T", s, k), peer, esend.at[k], erecv.at[s, k], erecv.at[s, k])

    def copy_of(key, arriving=False):
        place, src, dst, peer, got = mail[key]
        return pltpu.make_async_remote_copy(
            src_ref=got if arriving else src,
            dst_ref=got if arriving else dst,
            send_sem=send_sems.at[place],
            recv_sem=recv_sems.at[place],
            device_id=peer,
            device_id_type=MESH,
        )

    leaving, waited = [], set()

    def send(*keys):
        for key in keys:
            copy_of(key).start()
            leaving.append(key)

    def left(key):
        if key in leaving:
            copy_of(key).wait_send()
            leaving.remove(key)

    def run(way, s, piece):
        table, source, contract, partial = (0, eb[s], 0, seg_p) if way == "P" else (1, pb[s], 1, seg_e)
        groups = slots // UNROLL
        first, end = (-(-groups * k // PIECES) for k in (piece, piece + 1))

        def steps(group, total):
            for step in range(UNROLL):
                place = group * UNROLL + step
                product = lax.dot_general(
                    source[whole[table, 1, place]],
                    tiles[whole[table, 0, place]],
                    (((1,), (contract,)), ((), ())),
                    preferred_element_type=jnp.float32,
                )
                total = total * parts[table, 0, place] + product
                partial[place] = total
            return total

        start = partial[first * UNROLL - 1] if piece else jnp.zeros(partial.shape[1:], jnp.float32)
        lax.fori_loop(first, end, steps, start)

    def own_p(u, h):
        def value(i, k):
            block = 3 * u + i
            return seg_p[whole[0, 2, block], pl.ds(48 * h + 16 * k, 16), :] * parts[0, 1, block]

        return value

    def rows_of(i, k):
        return pl.ds(pl.multiple_of(48 * i + 16 * k, 16), 16)

    def own_e(block):
        def value(i, k):
            return seg_e[whole[1, 2, block], rows_of(i, k), :] * parts[1, 1, block]

        return value

    def pair_e(s, hh, zz):
        value = own_e(at_z(hh, zz, core))
        place = 4 * hh + zz
        return lambda i, k: value(i, k) + drecv[s, place, rows_of(i, k), :]

    def kept_e(place):
        return lambda i, k: kept[place, rows_of(i, k), :]

    def scale_of(ref, pieces):
        coded = ref[48 * pieces : 48 * pieces + 16, :].astype(jnp.int32).astype(jnp.float32)
        return jnp.exp2(coded * (1.0 / FINE)) * (1.0 / TOP)

    def over(pieces, carry, own, refs, visit):
        scales = [scale_of(ref, pieces) for ref in refs]

        def body(i, carry):
            for k in range(3):
                value = own(i, k)
                for ref, scale in zip(refs, scales):
                    value = value + ref[rows_of(i, k), :].astype(jnp.int32).astype(jnp.float32) * scale
                carry = visit(i, k, value, carry)
            return carry

        return lax.fori_loop(0, pieces, body, carry)

    def code(out, pieces, own, refs):
        def keep_it(i, k, value, most):
            tmp[rows_of(i, k), :] = value
            return jnp.maximum(most, jnp.abs(value))

        most = over(pieces, jnp.zeros((16, tmp.shape[1]), jnp.float32), own, refs, keep_it)
        level = jnp.ceil(jnp.log2(jnp.maximum(most, 1e-30)) * FINE)
        out[48 * pieces : 48 * pieces + 16, :] = level.astype(jnp.int32).astype(jnp.int16)
        scale = jnp.exp2(level * (-1.0 / FINE)) * TOP

        def body(i, carry):
            for k in range(3):
                out[rows_of(i, k), :] = jnp.round(tmp[rows_of(i, k), :] * scale).astype(jnp.int32).astype(jnp.int16)
            return carry

        lax.fori_loop(0, pieces, body, 0)

    owner_p = {
        "R8": (yo, xq), "R6": (ym, xq), "R7": (yp, xq), "R4": (yo, xl), "R5": (yo, xl),
        "R1": (y, xq), "R2": (ym, xl), "R3": (yp, xl),
    }
    owner_e = ((hq, zp), (hq, zm), (hq, zo), (xh, zp), (xh, zm), (xh, zo), (hq, z))

    def put_p(s, h, needs):
        if s == 0:
            pb[0][pl.ds(3 * el, 3), 48 * h : 48 * h + 48] = phon_dev[:, 48 * h : 48 * h + 48].astype(jnp.bfloat16)
            return

        def visit(i, k, value, carry):
            rows = pl.ds(48 * h + 16 * k, 16)
            total = phon_source[i, rows, :] + value
            if s < ITERS:
                pb[s][3 * el + i, rows, :] = (total / phon_rate[i]).astype(jnp.bfloat16)
            else:
                phon_out[i, rows, :] = total
            return carry

        over(3, 0, own_p(el, h), [mail[m][4] for m in needs], visit)

    def put_e(s, needs):
        if s == 0:
            eb[0][ph] = elec_dev[...].astype(jnp.bfloat16)
            return

        def visit(i, k, value, carry):
            rows = rows_of(i, k)
            total = elec_source[rows, :] + value
            if s < ITERS:
                eb[s][ph, rows, :] = (total / elec_rate[...]).astype(jnp.bfloat16)
            else:
                elec_out[rows, :] = total
            return carry

        over(2, 0, kept_e(0), [mail[m][4] for m in needs], visit)

    steps = plan()
    loaded = False
    for name, _, _ in steps.order():
        _, _, needs, sends = steps.steps[name]
        for m in needs:
            if m not in waited:
                copy_of(m, arriving=True).wait_recv()
                waited.add(m)
        kind, s = name[:2]
        if kind in ("P", "E"):
            if not loaded:
                for copy in table_copies + loads:
                    copy.wait()
                loaded = True
            run(kind, s, name[2])
        elif kind == "put_p":
            put_p(s, name[2], needs)
        elif kind == "put_e":
            put_e(s, needs)
        elif kind in P_SLOTS:
            h = name[2]
            left((kind, s - 1, h))
            code(psend.at[P_SLOTS[kind] + h], 3, own_p(at_y(*owner_p[kind]), h), [mail[m][4] for m in needs])
        elif kind == "D":
            left(("D", s - 1))
            for k in range(8):
                block = at_z(k // 4, k % 4, 1 - core)
                dsend[k] = seg_e[whole[1, 2, block]] * parts[1, 1, block]
        elif kind == "K":
            for k, hh in enumerate((xh, hq)):
                block = at_z(hh, z, core)
                kept[k] = seg_e[whole[1, 2, block]] * parts[1, 1, block] + drecv[s, 4 * hh + z]
        elif kind == "T":
            k = name[2]
            left(("T", s - 1, k))
            code(esend.at[k], 2, kept_e(1) if k == 6 else pair_e(s, *owner_e[k]), [mail[m][4] for m in needs if k == 6])
        send(*(m for m, _, _ in sends))
    for key in tuple(leaving):
        left(key)


def local(
    elec_dev, phon_dev, elec_source, phon_source, elec_rate, phon_rate, tiles, tile_rows, tile_cols, tile_count
):
    slots, side, _ = tiles.shape[2:]
    rhs = elec_dev.shape[1]
    vmem, smem = pl.BlockSpec(memory_space=pltpu.VMEM), pl.BlockSpec(memory_space=pltpu.SMEM)
    elec_sum, phon_sum = pl.pallas_call(
        kernel,
        out_shape=(
            jax.ShapeDtypeStruct((rhs, side), jnp.float32),
            jax.ShapeDtypeStruct((3, rhs, side), jnp.float32),
        ),
        in_specs=[smem, vmem, vmem, pl.BlockSpec(memory_space=pl.ANY)] + [vmem] * 6,
        out_specs=(vmem, vmem),
        scratch_shapes=[
            pltpu.VMEM((slots, side, side), jnp.bfloat16),
            pltpu.VMEM((slots, rhs, side), jnp.float32),
            pltpu.VMEM((slots, rhs, side), jnp.float32),
            *[pltpu.VMEM((24, rhs, side), jnp.bfloat16)] * ITERS,
            *[pltpu.VMEM((16, rhs, side), jnp.bfloat16)] * ITERS,
            pltpu.VMEM((14, 160, side), jnp.int16),
            pltpu.VMEM((ITERS, 14, 160, side), jnp.int16),
            pltpu.VMEM((8, rhs, side), jnp.float32),
            pltpu.VMEM((ITERS, 8, rhs, side), jnp.float32),
            pltpu.VMEM((7, 112, side), jnp.int16),
            pltpu.VMEM((ITERS, 7, 112, side), jnp.int16),
            pltpu.VMEM((2, rhs, side), jnp.float32),
            pltpu.VMEM((144, side), jnp.float32),
            pltpu.VMEM((2, 8, slots), jnp.int32),
            pltpu.VMEM((2, 8, slots), jnp.float32),
            pltpu.SMEM((2, 8, slots), jnp.int32),
            pltpu.SMEM((2, 8, slots), jnp.float32),
            pltpu.SemaphoreType.DMA((LOADS,)),
            pltpu.SemaphoreType.DMA((2,)),
            pltpu.SemaphoreType.DMA((ITERS * PER_SWEEP,)),
            pltpu.SemaphoreType.DMA((ITERS * PER_SWEEP,)),
        ],
        compiler_params=pltpu.CompilerParams(
            vmem_limit_bytes=62 * 2**20, collective_id=0, has_side_effects=True
        ),
        name="sweeps",
    )(
        tile_count,
        tile_rows[0],
        tile_cols[0],
        tiles[0, 0],
        elec_dev[0],
        phon_dev[0],
        elec_source[0],
        phon_source[0],
        elec_rate,
        phon_rate[0][:, None, :],
    )
    return elec_sum[None] / elec_rate[:, None, :], phon_sum[None] / phon_rate[:, :, None, :]


def solution(mesh):
    both = ("el", "ph")
    placed = (
        P(both, None, None),
        P("ph", "el", None, None),
        P(both, None, None),
        P("ph", "el", None, None),
        P(both, None),
        P("ph", "el", None),
        P("el", "ph", None, None, None),
        P("el", "ph", None),
        P("el", "ph", None),
        P("el", "ph"),
    )
    return jax.shard_map(
        local,
        mesh=mesh,
        in_specs=placed,
        out_specs=(P(both, None, None), P("ph", "el", None, None)),
        check_vma=False,
    )
```

```python
import random

import jax
import jax.numpy as jnp
from jax import lax
from jax.experimental import pallas as pl
from jax.experimental.pallas import tpu as pltpu
from jax.sharding import PartitionSpec as P

ITERS = 3
UNROLL = 8
LOADS = 8
PIECES = 5
TOP = 32000.0
FINE = 8.0
MESH = pl.DeviceIdType.MESH

WIRE = 46.7e3
HOP = {"x": 1.9, "y+": 2.0, "y-": 2.0, "z+": 2.0, "z-": 2.0, "zz": 2.5, "xx": 2.5, "d": 0.9}
LINK = {"x": "x", "xx": "x", "y+": "y+", "y-": "y-", "z+": "z+", "z-": "z-", "zz": "z+", "d": "d"}
LOAD = {"xx": 1.2, "zz": 1.2, "d": 0.07}
PASSES = (("P", 0), ("E", 0), ("E", 1), ("P", 1), ("P", 2), ("E", 2))
SEED = 0
SPREAD = 0.0
P_HALF, P_CODED, E_BLOCK, E_CODED = 3 * 48 * 512, 160 * 512, 96 * 512, 112 * 512


class Plan:
    def __init__(self):
        self.steps = {}

    def add(self, name, cost, after=(), needs=(), sends=()):
        self.steps[name] = (cost, tuple(after), tuple(needs), tuple(sends))

    def order(self):
        chance = random.Random(SEED)
        lean = {n: chance.uniform(1.0 - SPREAD, 1.0 + SPREAD) for n in self.steps}
        sender = {m: (n, way, size) for n, (_, _, _, sends) in self.steps.items() for m, way, size in sends}
        users = {n: [] for n in self.steps}
        for name, (_, after, needs, _) in self.steps.items():
            for n in after:
                users[n].append((name, 0.0))
            for m in needs:
                n, way, size = sender[m]
                users[n].append((name, HOP[way] + size * LOAD.get(way, 1.0) / WIRE))
        tail = {}

        def rest(name):
            if name not in tail:
                cost = self.steps[name][0]
                tail[name] = cost + max((gap + rest(n) for n, gap in users[name]), default=0.0)
            return tail[name]

        now, free, arrival, done, result = 0.0, {}, {}, set(), []
        left = dict.fromkeys(self.steps)
        while left:
            ready = []
            for name in left:
                _, after, needs, _ = self.steps[name]
                if all(n in done for n in after) and all(m in arrival for m in needs):
                    urgent = 1000.0 if self.steps[name][0] < 0.04 else 0.0
                    ready.append((max([now] + [arrival[m] for m in needs]), -rest(name) * lean[name] - urgent, name))
            soonest = min(ready)[0]
            start, _, name = min((r for r in ready if r[0] <= max(now, soonest) + 0.05), key=lambda r: r[1])
            cost, _, _, sends = self.steps[name]
            now = start + cost
            for m, way, size in sends:
                link = LINK[way]
                begin = max(now, free.get(link, 0.0))
                free[link] = begin + size * LOAD.get(way, 1.0) / WIRE
                arrival[m] = free[link] + HOP[way]
            done.add(name)
            del left[name]
            result.append((name, start, now))
        return result


def plan():
    p = Plan()
    for s in range(ITERS):
        if s == 0:
            p.add(("put_e", 0), 0.05, (), (), e_first(0))
            for h in range(2):
                p.add(("put_p", 0, h), 0.05, (("put_e", 0),), (), p_first(0, h))
        own_p = [("put_p", s, h) for h in range(2)]
        for m, by, way, h in (("AHP", "AYP", "y+", 0), ("AHM", "AYM", "y-", 1)):
            p.add((m, s), 0.01, (), ((by, s, h),), (((m, s), way, P_HALF),))
        for h, by in ((0, "AHP"), (1, "AHM")):
            p.add(("AQ", s, h), 0.02, (), (("AX", s, h),), ((("AQP", s, h), "y+", P_HALF), (("AQM", s, h), "y-", P_HALF)))
            p.add(("AOX", s, h), 0.01, (), ((by, s),), ((("AOX", s, h), "x", P_HALF),))
        p.add(("F", s), 0.03, (), (("G", s, 0),), e_onward(s))
        for k, by in ((9, 1), (10, 2), (11, 3), (12, 4), (13, 5), (14, 6)):
            p.add(("S", s, k), 0.01, (), (("G", s, by),), ((("G", s, k), "d", E_BLOCK),))
        all_p = [(m, s, h) for m in ("AX", "AYP", "AYM", "AQP", "AQM", "AOX") for h in range(2)]
        all_p += [("AHP", s), ("AHM", s)]
        all_e = [("G", s, k) for k in range(15)]
        for k in range(PIECES):
            for way, arrived, extra in (("P", all_e, [("put_e", s)]), ("E", all_p, own_p)):
                if k:
                    p.add((way, s, k), (P_TIME if way == "P" else E_TIME) / PIECES, ((way, s, k - 1),))
                else:
                    old = [n for n in p.steps if n[1] == s - 1 and n[0] in (P_CODES if way == "P" else E_CODES)]
                    old = [n for n in old if n != ("T", s - 1, 6)]
                    if way == "P" and s:
                        old += own_p
                    p.add((way, s, k), (P_TIME if way == "P" else E_TIME) / PIECES, old + extra, arrived)
        last_p, last_e = (("P", s, PIECES - 1),), (("E", s, PIECES - 1),)
        for h in range(2):
            for m, way in (("R8", "x"), ("R6", "y-"), ("R7", "y+")):
                p.add((m, s, h), 0.13, last_p, (), (((m, s, h), way, P_CODED),))
        p.add(("R4", s, 0), 0.14, last_p, (("R8", s, 0),), ((("R4", s, 0), "y-", P_CODED),))
        p.add(("R5", s, 1), 0.14, last_p, (("R8", s, 1),), ((("R5", s, 1), "y+", P_CODED),))
        for h in range(2):
            p.add(("R1", s, h), 0.15, last_p, (("R6", s, h), ("R7", s, h)), ((("R1", s, h), "x", P_CODED),))
            low, high = ((("R4", s, 0),), ()) if h == 0 else ((), (("R5", s, 1),))
            p.add(("R2", s, h), 0.14, last_p + ((("R4", s, 0),) if h else ()), low, ((("R2", s, h), "y-", P_CODED),))
            p.add(("R3", s, h), 0.14, last_p + (() if h else (("R5", s, 1),)), high, ((("R3", s, h), "y+", P_CODED),))
            p.add(
                ("put_p", s + 1, h), 0.15, last_p, (("R1", s, h), ("R2", s, h), ("R3", s, h)),
                p_first(s + 1, h) if s + 1 < ITERS else (),
            )
        p.add(("D", s), 0.3, last_e, (), ((("D", s), "d", 16 * E_BLOCK),))
        for k, way in enumerate(("z+", "z-", "zz", "z+", "z-", "zz")):
            p.add(("T", s, k), 0.09, last_e, (("D", s),), ((("T", s, k), way, E_CODED),))
        before = (("put_e", s),)
        p.add(("K", s), 0.08, last_e + before, (("D", s),))
        p.add(("T", s, 6), 0.12, (("K", s),), [("T", s, k) for k in range(3)], ((("T", s, 6), "xx", E_CODED),))
        p.add(
            ("put_e", s + 1), 0.15, (("K", s), ("T", s, 6)), [("T", s, k) for k in range(3, 7)],
            e_first(s + 1) if s + 1 < ITERS else (),
        )
    for before, name in zip(PASSES, PASSES[1:]):
        cost, after, needs, sends = p.steps[name + (0,)]
        p.steps[name + (0,)] = (cost, after + (before + (PIECES - 1,),), needs, sends)
    return p


P_TIME, E_TIME = 5.1, 7.5
P_CODES, E_CODES = ("R8", "R6", "R7", "R4", "R5", "R1", "R2", "R3"), ("D", "T", "K")


def e_first(s):
    ways = ("xx", "z+", "z-", "zz")
    return tuple((("G", s, k), way, E_BLOCK) for k, way in enumerate(ways)) + ((("G", s, 7), "d", E_BLOCK),)


def e_onward(s):
    ways = ("z+", "z-", "zz")
    return tuple((("G", s, 4 + k), way, E_BLOCK) for k, way in enumerate(ways)) + ((("G", s, 8), "d", E_BLOCK),)


def p_first(s, h):
    return tuple(((m, s, h), way, P_HALF) for m, way in (("AX", "x"), ("AYP", "y+"), ("AYM", "y-")))


def tables_of(own, other, live, blocks, whole, parts):
    slots = own.shape[1]
    square = (slots, slots)
    here = lax.broadcasted_iota(jnp.int32, square, 1)
    there = lax.broadcasted_iota(jnp.int32, square, 0)

    def down(row):
        return jnp.broadcast_to(row, square).T

    block = jnp.where(live, own, blocks)
    key = block * slots + here[0:1]
    rank = jnp.sum((down(key) < key).astype(jnp.int32), axis=0, keepdims=True)
    place = down(rank)
    block_down = down(block)

    def moved(values, by):
        return jnp.sum(jnp.where(place + by == here, values, 0), axis=0, keepdims=True)

    whole[0:1, :] = moved(there, 0)
    whole[1:2, :] = moved(down(jnp.where(live, other, 0)), 0)
    up_to = jnp.sum((block_down <= here).astype(jnp.int32), axis=0, keepdims=True)
    whole[2:3, :] = jnp.maximum(jnp.where(here[0:1] < blocks, up_to, 1) - 1, 0)
    parts[0:1, :] = (moved(block_down + 1, 0) == moved(block_down + 1, 1)).astype(jnp.float32)
    has = jnp.sum((block_down == here).astype(jnp.int32), axis=0, keepdims=True)
    parts[1:2, :] = (has > 0).astype(jnp.float32)


PER_SWEEP = 51
P_SLOTS = {"R8": 0, "R6": 2, "R7": 4, "R4": 6, "R5": 6, "R1": 8, "R2": 10, "R3": 12}


def kernel(
    count, slot_rows, slot_cols, tiles_hbm, elec_dev, phon_dev, elec_source, phon_source, elec_rate, phon_rate,
    sums,
    tiles, seg_p, seg_e, pb_0, pb_1, pb_2, eb_0, eb_1, eb_2, psend, precv, dsend, drecv, esend, erecv, kept, tmp,
    whole_v, parts_v, whole, parts, load_sems, table_sems, send_sems, recv_sems,
):
    pb, eb = (pb_0, pb_1, pb_2), (eb_0, eb_1, eb_2)
    slots = tiles.shape[0]
    part = slots // LOADS
    loads = [
        pltpu.make_async_copy(tiles_hbm.at[pl.ds(part * i, part)], tiles.at[pl.ds(part * i, part)], load_sems.at[i])
        for i in range(LOADS)
    ]
    el, ph = lax.axis_index("el"), lax.axis_index("ph")
    y, xl = lax.div(el, 2), lax.rem(el, 2)
    yp, ym, yo, xq = lax.rem(y + 1, 4), lax.rem(y + 3, 4), lax.rem(y + 2, 4), 1 - xl
    xh, z, core = lax.div(ph, 8), lax.rem(lax.div(ph, 2), 4), lax.rem(ph, 2)
    zp, zm, zo, hq = lax.rem(z + 1, 4), lax.rem(z + 3, 4), lax.rem(z + 2, 4), 1 - xh

    def at_y(yy, xx):
        return 2 * yy + xx

    def at_z(hh, zz, cc):
        return 8 * hh + 2 * zz + cc

    p_x, p_yp, p_ym = (at_y(y, xq), ph), (at_y(yp, xl), ph), (at_y(ym, xl), ph)
    sib = (el, at_z(xh, z, 1 - core))
    e_zp, e_zm, e_zo, e_x = (
        (el, at_z(xh, zp, core)),
        (el, at_z(xh, zm, core)),
        (el, at_z(xh, zo, core)),
        (el, at_z(hq, z, core)),
    )

    barrier = pltpu.get_barrier_semaphore()
    for peer in (p_x, p_yp, p_ym, sib, e_zp, e_zm, e_zo, e_x):
        pl.semaphore_signal(barrier, inc=1, device_id=peer, device_id_type=MESH)
    for load in loads:
        load.start()

    live = lax.broadcasted_iota(jnp.int32, (1, slots), 1) < count[0, 0]
    table_copies = []
    for i, (own, other, blocks) in enumerate(((slot_cols, slot_rows, 24), (slot_rows, slot_cols, 16))):
        tables_of(own[...], other[...], live, blocks, whole_v.at[i], parts_v.at[i])
    for i, (src, dst) in enumerate(((whole_v, whole), (parts_v, parts))):
        table_copies.append(pltpu.make_async_copy(src, dst, table_sems.at[i]))
        table_copies[-1].start()
    pl.semaphore_wait(barrier, 8)

    def unit(s, h, yy, xx):
        return pb[s].at[pl.ds(3 * at_y(yy, xx), 3), pl.ds(48 * h, 48)]

    def eblock(s, hh, zz, cc):
        return eb[s].at[at_z(hh, zz, cc)]

    mail = {}

    def route(key, peer, src, dst, got):
        mail[key] = (len(mail), src, dst, peer, got)

    for s in range(ITERS):
        for h in range(2):
            for name, peer, sent, got in (
                ("AX", p_x, (y, xl), (y, xq)),
                ("AYP", p_yp, (y, xl), (ym, xl)),
                ("AYM", p_ym, (y, xl), (yp, xl)),
                ("AQP", p_yp, (y, xq), (ym, xq)),
                ("AQM", p_ym, (y, xq), (yp, xq)),
                ("AOX", p_x, (yo, xl), (yo, xq)),
            ):
                route((name, s, h), peer, unit(s, h, *sent), unit(s, h, *sent), unit(s, h, *got))
            for name, peer in (
                ("R8", p_x), ("R6", p_ym), ("R7", p_yp), ("R1", p_x), ("R2", p_ym), ("R3", p_yp),
                ("R5" if h else "R4", p_yp if h else p_ym),
            ):
                slot = P_SLOTS[name] + h
                route((name, s, h), peer, psend.at[slot], precv.at[s, slot], precv.at[s, slot])
        route(("AHP", s), p_yp, unit(s, 0, ym, xl), unit(s, 0, ym, xl), unit(s, 0, yo, xl))
        route(("AHM", s), p_ym, unit(s, 1, yp, xl), unit(s, 1, yp, xl), unit(s, 1, yo, xl))
        own = eblock(s, xh, z, core)
        far = eblock(s, hq, z, core)
        route(("G", s, 0), e_x, own, own, far)
        for k, (peer, came) in enumerate(((e_zp, zm), (e_zm, zp), (e_zo, zo))):
            route(("G", s, 1 + k), peer, own, own, eblock(s, xh, came, core))
            route(("G", s, 4 + k), peer, far, far, eblock(s, hq, came, core))
        for k, at in enumerate(((xh, z), (hq, z), (xh, zm), (xh, zp), (xh, zo), (hq, zm), (hq, zp), (hq, zo))):
            route(("G", s, 7 + k), sib, eblock(s, *at, core), eblock(s, *at, core), eblock(s, *at, 1 - core))
        route(("D", s), sib, dsend, drecv.at[s], drecv.at[s])
        for k, peer in enumerate((e_zp, e_zm, e_zo, e_zp, e_zm, e_zo, e_x)):
            route(("T", s, k), peer, esend.at[k], erecv.at[s, k], erecv.at[s, k])

    def copy_of(key, arriving=False):
        place, src, dst, peer, got = mail[key]
        return pltpu.make_async_remote_copy(
            src_ref=got if arriving else src,
            dst_ref=got if arriving else dst,
            send_sem=send_sems.at[place],
            recv_sem=recv_sems.at[place],
            device_id=peer,
            device_id_type=MESH,
        )

    leaving, waited = [], set()

    def send(*keys):
        for key in keys:
            copy_of(key).start()
            leaving.append(key)

    def left(key):
        if key in leaving:
            copy_of(key).wait_send()
            leaving.remove(key)

    def run(way, s, piece):
        table, source, contract, partial = (0, eb[s], 0, seg_p) if way == "P" else (1, pb[s], 1, seg_e)
        groups = slots // UNROLL
        first, end = (-(-groups * k // PIECES) for k in (piece, piece + 1))

        def steps(group, total):
            for step in range(UNROLL):
                place = group * UNROLL + step
                product = lax.dot_general(
                    source[whole[table, 1, place]],
                    tiles[whole[table, 0, place]],
                    (((1,), (contract,)), ((), ())),
                    preferred_element_type=jnp.float32,
                )
                total = total * parts[table, 0, place] + product
                partial[place] = total
            return total

        start = partial[first * UNROLL - 1] if piece else jnp.zeros(partial.shape[1:], jnp.float32)
        lax.fori_loop(first, end, steps, start)

    def own_p(u, h):
        def value(i, k):
            block = 3 * u + i
            return seg_p[whole[0, 2, block], pl.ds(48 * h + 16 * k, 16), :] * parts[0, 1, block]

        return value

    def rows_of(i, k):
        return pl.ds(pl.multiple_of(48 * i + 16 * k, 16), 16)

    def own_e(block):
        def value(i, k):
            return seg_e[whole[1, 2, block], rows_of(i, k), :] * parts[1, 1, block]

        return value

    def pair_e(s, hh, zz):
        value = own_e(at_z(hh, zz, core))
        place = 4 * hh + zz
        return lambda i, k: value(i, k) + drecv[s, place, rows_of(i, k), :]

    def kept_e(place):
        return lambda i, k: kept[place, rows_of(i, k), :]

    def scale_of(ref, pieces):
        coded = ref[48 * pieces : 48 * pieces + 16, :].astype(jnp.int32).astype(jnp.float32)
        return jnp.exp2(coded * (1.0 / FINE)) * (1.0 / TOP)

    def over(pieces, carry, own, refs, visit):
        scales = [scale_of(ref, pieces) for ref in refs]

        def body(i, carry):
            for k in range(3):
                value = own(i, k)
                for ref, scale in zip(refs, scales):
                    value = value + ref[rows_of(i, k), :].astype(jnp.int32).astype(jnp.float32) * scale
                carry = visit(i, k, value, carry)
            return carry

        return lax.fori_loop(0, pieces, body, carry)

    def code(out, pieces, own, refs):
        def keep_it(i, k, value, most):
            tmp[rows_of(i, k), :] = value
            return jnp.maximum(most, jnp.abs(value))

        most = over(pieces, jnp.zeros((16, tmp.shape[1]), jnp.float32), own, refs, keep_it)
        level = jnp.ceil(jnp.log2(jnp.maximum(most, 1e-30)) * FINE)
        out[48 * pieces : 48 * pieces + 16, :] = level.astype(jnp.int32).astype(jnp.int16)
        scale = jnp.exp2(level * (-1.0 / FINE)) * TOP

        def body(i, carry):
            for k in range(3):
                out[rows_of(i, k), :] = jnp.round(tmp[rows_of(i, k), :] * scale).astype(jnp.int32).astype(jnp.int16)
            return carry

        lax.fori_loop(0, pieces, body, 0)

    owner_p = {
        "R8": (yo, xq), "R6": (ym, xq), "R7": (yp, xq), "R4": (yo, xl), "R5": (yo, xl),
        "R1": (y, xq), "R2": (ym, xl), "R3": (yp, xl),
    }
    owner_e = ((hq, zp), (hq, zm), (hq, zo), (xh, zp), (xh, zm), (xh, zo), (hq, z))

    def put_p(s, h, needs):
        if s == 0:
            pb[0][pl.ds(3 * el, 3), 48 * h : 48 * h + 48] = phon_dev[:, 48 * h : 48 * h + 48].astype(jnp.bfloat16)
            return

        def visit(i, k, value, carry):
            rows = pl.ds(48 * h + 16 * k, 16)
            total = phon_source[i, rows, :] + value
            if s < ITERS:
                pb[s][3 * el + i, rows, :] = (total / phon_rate[i]).astype(jnp.bfloat16)
            else:
                sums[1 + i, rows, :] = total
            return carry

        over(3, 0, own_p(el, h), [mail[m][4] for m in needs], visit)

    def put_e(s, needs):
        if s == 0:
            eb[0][ph] = elec_dev[...].astype(jnp.bfloat16)
            return

        def visit(i, k, value, carry):
            rows = rows_of(i, k)
            total = elec_source[rows, :] + value
            if s < ITERS:
                eb[s][ph, rows, :] = (total / elec_rate[...]).astype(jnp.bfloat16)
            else:
                sums[0, rows, :] = total
            return carry

        over(2, 0, kept_e(0), [mail[m][4] for m in needs], visit)

    steps = plan()
    loaded = False
    for name, _, _ in steps.order():
        _, _, needs, sends = steps.steps[name]
        for m in needs:
            if m not in waited:
                copy_of(m, arriving=True).wait_recv()
                waited.add(m)
        kind, s = name[:2]
        if kind in ("P", "E"):
            if not loaded:
                for copy in table_copies + loads:
                    copy.wait()
                loaded = True
            run(kind, s, name[2])
        elif kind == "put_p":
            put_p(s, name[2], needs)
        elif kind == "put_e":
            put_e(s, needs)
        elif kind in P_SLOTS:
            h = name[2]
            left((kind, s - 1, h))
            code(psend.at[P_SLOTS[kind] + h], 3, own_p(at_y(*owner_p[kind]), h), [mail[m][4] for m in needs])
        elif kind == "D":
            left(("D", s - 1))
            for k in range(8):
                block = at_z(k // 4, k % 4, 1 - core)
                dsend[k] = seg_e[whole[1, 2, block]] * parts[1, 1, block]
        elif kind == "K":
            for k, hh in enumerate((xh, hq)):
                block = at_z(hh, z, core)
                kept[k] = seg_e[whole[1, 2, block]] * parts[1, 1, block] + drecv[s, 4 * hh + z]
        elif kind == "T":
            k = name[2]
            left(("T", s - 1, k))
            code(esend.at[k], 2, kept_e(1) if k == 6 else pair_e(s, *owner_e[k]), [mail[m][4] for m in needs if k == 6])
        send(*(m for m, _, _ in sends))
    for key in tuple(leaving):
        left(key)


def finish(sums, elec_rate, phon_rate, elec_out, phon_out):
    elec_out[...] = sums[0] / elec_rate[...]
    for block in range(phon_out.shape[0]):
        phon_out[block] = sums[1 + block] / phon_rate[block]


def local(
    elec_dev, phon_dev, elec_source, phon_source, elec_rate, phon_rate, tiles, tile_rows, tile_cols, tile_count
):
    slots, side, _ = tiles.shape[2:]
    rhs = elec_dev.shape[1]
    vmem, smem = pl.BlockSpec(memory_space=pltpu.VMEM), pl.BlockSpec(memory_space=pltpu.SMEM)
    sums = pl.pallas_call(
        kernel,
        out_shape=jax.ShapeDtypeStruct((4, rhs, side), jnp.float32),
        in_specs=[smem, vmem, vmem, pl.BlockSpec(memory_space=pl.ANY)] + [vmem] * 6,
        out_specs=vmem,
        scratch_shapes=[
            pltpu.VMEM((slots, side, side), jnp.bfloat16),
            pltpu.VMEM((slots, rhs, side), jnp.float32),
            pltpu.VMEM((slots, rhs, side), jnp.float32),
            *[pltpu.VMEM((24, rhs, side), jnp.bfloat16)] * ITERS,
            *[pltpu.VMEM((16, rhs, side), jnp.bfloat16)] * ITERS,
            pltpu.VMEM((14, 160, side), jnp.int16),
            pltpu.VMEM((ITERS, 14, 160, side), jnp.int16),
            pltpu.VMEM((8, rhs, side), jnp.float32),
            pltpu.VMEM((ITERS, 8, rhs, side), jnp.float32),
            pltpu.VMEM((7, 112, side), jnp.int16),
            pltpu.VMEM((ITERS, 7, 112, side), jnp.int16),
            pltpu.VMEM((2, rhs, side), jnp.float32),
            pltpu.VMEM((144, side), jnp.float32),
            pltpu.VMEM((2, 8, slots), jnp.int32),
            pltpu.VMEM((2, 8, slots), jnp.float32),
            pltpu.SMEM((2, 8, slots), jnp.int32),
            pltpu.SMEM((2, 8, slots), jnp.float32),
            pltpu.SemaphoreType.DMA((LOADS,)),
            pltpu.SemaphoreType.DMA((2,)),
            pltpu.SemaphoreType.DMA((ITERS * PER_SWEEP,)),
            pltpu.SemaphoreType.DMA((ITERS * PER_SWEEP,)),
        ],
        compiler_params=pltpu.CompilerParams(
            vmem_limit_bytes=62 * 2**20, collective_id=0, has_side_effects=True
        ),
        name="sweeps",
    )(
        tile_count,
        tile_rows[0],
        tile_cols[0],
        tiles[0, 0],
        elec_dev[0],
        phon_dev[0],
        elec_source[0],
        phon_source[0],
        elec_rate,
        phon_rate[0][:, None, :],
    )
    elec_out, phon_out = pl.pallas_call(
        finish,
        out_shape=(
            jax.ShapeDtypeStruct((rhs, side), jnp.float32),
            jax.ShapeDtypeStruct((3, rhs, side), jnp.float32),
        ),
        in_specs=[vmem] * 3,
        out_specs=(vmem, vmem),
        compiler_params=pltpu.CompilerParams(vmem_limit_bytes=8 * 2**20),
        name="finish",
    )(sums, elec_rate, phon_rate[0][:, None, :])
    return elec_out[None], phon_out[None]


def solution(mesh):
    both = ("el", "ph")
    placed = (
        P(both, None, None),
        P("ph", "el", None, None),
        P(both, None, None),
        P("ph", "el", None, None),
        P(both, None),
        P("ph", "el", None),
        P("el", "ph", None, None, None),
        P("el", "ph", None),
        P("el", "ph", None),
        P("el", "ph"),
    )
    return jax.shard_map(
        local,
        mesh=mesh,
        in_specs=placed,
        out_specs=(P(both, None, None), P("ph", "el", None, None)),
        check_vma=False,
    )
```
